32 devices in a mesh: dp: 4 (over z), row: 4 (over x, core), col: 2 (over y).
Axes of the slice: x: 2, y: 2, z: 4, core: 2. Of those that a mesh axis runs over, the one named last changes fastest.
Arguments:
- inputs: bfloat16 [4096, 2048], P(('dp', 'row'), 'col'), may hold values from -6 to 6
- heads_weight: bfloat16 [2048, 4096], P('col', 'row'), may hold values from -0.125 to 0.125
- output_weight: bfloat16 [2048, 2048], P('row', 'col'), may hold values from -0.5 to 0.5
- gateup_weight: bfloat16 [2048, 12288], P('col', 'row'), may hold values from -0.125 to 0.125
- down_weight: bfloat16 [6144, 2048], P('row', 'col'), may hold values from -0.078125 to 0.078125
- first_gain: float32 [2048], P('col'), may hold values from 0.1 to 1.9
- second_gain: float32 [2048], P('col'), may hold values from 0.1 to 1.9
- query_gain: float32 [128], replicated, may hold values from 0.6 to 2.4
- key_gain: float32 [128], replicated, may hold values from 0.6 to 2.4
- segments: int32 [4096], P('dp'), may hold values from 0 to 7, as said below
- positions: int32 [4096], P('dp'), may hold values from 0 to 3071, as said below
- cotangent: bfloat16 [4096, 2048], P(('dp', 'row'), 'col'), may hold values from -6 to 6
Outputs:
- outputs: bfloat16 [4096, 2048], P(('dp', 'row'), 'col')
- input_grad: bfloat16 [4096, 2048], P(('dp', 'row'), 'col')
- heads_grad: float32 [2048, 4096], P('col', 'row')
- output_grad: float32 [2048, 2048], P('row', 'col')
- gateup_grad: float32 [2048, 12288], P('col', 'row')
- down_grad: float32 [6144, 2048], P('row', 'col')
- first_grad: float32 [2048], P('col')
- second_grad: float32 [2048], P('col')
- querygain_grad: float32 [128], replicated
- keygain_grad: float32 [128], replicated
The draws below stay inside these ranges and needn't reach their ends.
Inputs may be any that keep to these rules, and one draw needn't show every extreme that they name: `segments`: within each aligned block of 1024 tokens the numbers start at 0 and rise by 0 or 1 from one token to the next; equal numbers mark one document; a sequence holds 1 to 8 documents. `positions`: along a document the position rises by one from each token to the next.
All inputs are finite; a program needn't handle non-finite values.
Results may differ from the reference program's by a relative error of at most 0.015.
Values may be sent and summed in bfloat16 or wider, within the bound.
A program may use at most 192 MiB of HBM per device.

```python
import math
import jax
import jax.numpy as jnp
from jax import lax

D = 2048
HEADS = 16
KV_HEADS = 8
HEAD = 128
FF = 6144
SEQ_LEN = 1024
TOKENS = 4096


def doc_layout(key):
    base = jax.random.fold_in(key, 7)
    seq_total = TOKENS // SEQ_LEN
    spots = jnp.arange(SEQ_LEN).astype(jnp.int32)
    scores = jax.random.randint(jax.random.fold_in(base, 1), (seq_total, SEQ_LEN - 1), 0, 1048576).astype(jnp.int32)
    scores = scores * SEQ_LEN + jnp.arange(SEQ_LEN - 1).astype(jnp.int32)[None, :]
    best, picked = lax.top_k(scores, 7)
    picked = picked.astype(jnp.int32) + 1
    counts = jax.random.randint(jax.random.fold_in(base, 3), (seq_total,), 0, 8).astype(jnp.int32)
    counts = jnp.where(jnp.arange(seq_total).astype(jnp.int32) == 0, 7, counts).astype(jnp.int32)
    used = jnp.arange(7).astype(jnp.int32)[None, :] < counts[:, None]
    hits = (picked[:, :, None] == spots[None, None, :]) & used[:, :, None]
    starts = jnp.any(hits, axis=1) | (spots[None, :] == 0)
    segment_ids = jnp.cumsum(starts.astype(jnp.int32), axis=1).astype(jnp.int32) - 1
    first_spot = lax.cummax(jnp.where(starts, spots[None, :], 0).astype(jnp.int32), axis=1)
    shifts = jax.random.randint(jax.random.fold_in(base, 2), (seq_total, SEQ_LEN), 0, 2048).astype(jnp.int32)
    rows = jnp.arange(seq_total).astype(jnp.int32)[:, None]
    shifts = jnp.where(rows == 0, 2047 + spots[None, :], shifts).astype(jnp.int32)
    shifts = jnp.where(rows == 1, 0, shifts).astype(jnp.int32)
    offsets = jnp.take_along_axis(shifts, first_spot, axis=1)
    places = spots[None, :] - first_spot + offsets
    return (segment_ids.reshape(-1).astype(jnp.int32), places.reshape(-1).astype(jnp.int32))


def draw_segments(key, part):
    return doc_layout(key)[0]


def draw_positions(key, part):
    return doc_layout(key)[1]


def gain_values(key):
    spread = jax.random.uniform(key, (HEAD,), jnp.float32)
    spread = jnp.where(jnp.arange(HEAD) == 0, 0.0, jnp.where(jnp.arange(HEAD) == 1, 1.0, spread))
    return 0.6 + 1.8 * spread


def draw_query_gain(key, part):
    return gain_values(jax.random.fold_in(key, 11))


def draw_key_gain(key, part):
    return gain_values(jax.random.fold_in(key, 12))


def block_scale(key, dims, shards, least, top_value):
    loudness, own = 1.0, jax.random.fold_in(key, 6)
    for dim, shards_of in shards:
        heights = jnp.exp(jax.random.uniform(jax.random.fold_in(own, dim), (shards_of,), jnp.float32, least / len(shards), top_value / len(shards)))
        loudness = loudness * jnp.repeat(heights, dims[dim] // shards_of).reshape([-1 if axis == dim else 1 for axis in range(len(dims))])
    return loudness


def noise(key, shape, scale, limit, cuts=(), kind=jnp.bfloat16):
    factor_of = block_scale(key, shape, cuts, -0.22, 0.18) if cuts else 1.0
    entries = jax.random.normal(key, shape, jnp.float32) * scale * factor_of
    return jnp.minimum(jnp.maximum(entries, -limit), limit).astype(kind)


def setup_inputs(seed: int = 0) -> dict:
    streams_of = jax.random.split(jax.random.key(seed), 13)
    inputs = noise(streams_of[0], (TOKENS, D), 1.0, 6.0, ((0, 16), (1, 2)))
    heads_weight = noise(streams_of[1], (D, 4 * KV_HEADS * HEAD), D ** -0.5, 0.125, ((0, 2), (1, 4)))
    output_weight = noise(streams_of[2], (HEADS * HEAD, D), HEAD ** -0.5, 0.5, ((0, 4), (1, 2)))
    gateup_weight = noise(streams_of[3], (D, 2 * FF), D ** -0.5, 0.125, ((0, 2), (1, 4)))
    down_weight = noise(streams_of[4], (FF, D), FF ** -0.5, 0.078125, ((0, 4), (1, 2)))
    first_gain = jnp.clip(1.0 + 0.18 * jax.random.normal(streams_of[5], (D,), jnp.float32), 0.1, 1.9)
    second_gain = jnp.clip(1.0 + 0.18 * jax.random.normal(streams_of[6], (D,), jnp.float32), 0.1, 1.9)
    query_gain = draw_query_gain(jax.random.fold_in(streams_of[12], 71), 0)
    key_gain = draw_key_gain(jax.random.fold_in(streams_of[12], 71), 0)
    segments = draw_segments(jax.random.fold_in(streams_of[12], 71), 0)
    positions = draw_positions(jax.random.fold_in(streams_of[12], 71), 0)
    cotangent = noise(streams_of[11], (TOKENS, D), 1.0, 6.0, ((0, 16), (1, 2)))
    return dict(inputs=inputs, heads_weight=heads_weight, output_weight=output_weight, gateup_weight=gateup_weight, down_weight=down_weight, first_gain=first_gain, second_gain=second_gain, query_gain=query_gain, key_gain=key_gain, segments=segments, positions=positions, cotangent=cotangent)


epsilon = 1e-06
log_theta = math.log(1000000.0)
highest = lax.Precision.HIGHEST

@jax.custom_vjp
def low(v):
    return lax.optimization_barrier(v.astype(jnp.bfloat16)).astype(jnp.float32)

@jax.custom_vjp
def low_back(v):
    return v

def low_keep(v):
    return (low(v), None)

def low_pass(kept, grad):
    return (grad,)

def back_keep(v):
    return (v, None)

def back_low(kept, grad):
    return (low(grad),)
low.defvjp(low_keep, low_pass)
low_back.defvjp(back_keep, back_low)

def rms_norm(values, gain):
    return values * lax.rsqrt(lax.optimization_barrier(jnp.mean(values * values, axis=-1, keepdims=True)) + epsilon) * gain

def tables(positions, head_size):
    half_size = head_size // 2
    freqs = jnp.exp(-log_theta * jnp.arange(half_size).astype(jnp.float32) * 2.0 / head_size)
    angles = positions.astype(jnp.float32)[:, None] * freqs[None, :]
    return (jnp.cos(angles), jnp.sin(angles))

def rotate(values, cosine, sine):
    half_size = values.shape[-1] // 2
    first_half = values[..., :half_size]
    second_half = values[..., half_size:]
    return jnp.concatenate([first_half * cosine - second_half * sine, second_half * cosine + first_half * sine], axis=-1)

def sequence_attention(packed, segment, position, query_gain, key_gain):
    length = packed.shape[0]
    pieces = packed.reshape(length, KV_HEADS, 4, HEAD)
    cosine, sine = tables(position, HEAD)
    queries = rotate(rms_norm(pieces[:, :, 0:2], query_gain), cosine[:, None, None], sine[:, None, None])
    keys_rot = rotate(rms_norm(pieces[:, :, 2], key_gain), cosine[:, None], sine[:, None])
    values = pieces[:, :, 3]
    queries = low(queries)
    keys_rot = low(keys_rot)
    values = low(values)
    scores = jnp.einsum('ikgd,jkd->kgij', queries, keys_rot, precision=highest) * (1.0 / math.sqrt(HEAD))
    scores = low_back(scores)
    places = jnp.arange(length)
    allowed = (places[None, :] <= places[:, None]) & (segment[None, :] == segment[:, None])
    scores = jnp.where(allowed, scores, -1e+30)
    peak = lax.optimization_barrier(jnp.max(scores, axis=-1, keepdims=True))
    weights = jnp.exp(scores - peak)
    probs = weights / lax.optimization_barrier(jnp.sum(weights, axis=-1, keepdims=True))
    mixed = jnp.einsum('kgij,jkd->ikgd', low(probs), values, precision=highest)
    return mixed.reshape(length, HEADS * HEAD)

def layer(inputs, heads_weight, output_weight, gateup_weight, down_weight, first_gain, second_gain, query_gain, key_gain, segments, positions):
    token_count = inputs.shape[0]
    normed = low(rms_norm(inputs, first_gain))
    packed = low_back(jnp.dot(normed, heads_weight, precision=highest))
    seq_count = token_count // SEQ_LEN

    def one_sequence(item):
        return sequence_attention(item[0], item[1], item[2], query_gain, key_gain)
    attended = lax.map(jax.checkpoint(one_sequence), (packed.reshape(seq_count, SEQ_LEN, -1), segments.reshape(seq_count, SEQ_LEN), positions.reshape(seq_count, SEQ_LEN)))
    attended = attended.reshape(token_count, HEADS * HEAD)
    attended = low(low_back(attended))
    middle = inputs + low_back(jnp.dot(attended, output_weight, precision=highest))
    normed_two = low(rms_norm(middle, second_gain))
    gate_up = low_back(jnp.dot(normed_two, gateup_weight, precision=highest))
    gate_up = gate_up.reshape(token_count, KV_HEADS, 2, FF // KV_HEADS)
    hidden = low(jax.nn.silu(gate_up[:, :, 0]) * gate_up[:, :, 1]).reshape(token_count, FF)
    return middle + low_back(jnp.dot(hidden, down_weight, precision=highest))

def reference(inputs, heads_weight, output_weight, gateup_weight, down_weight, first_gain, second_gain, query_gain, key_gain, segments, positions, cotangent):
    floats = (inputs.astype(jnp.float32), heads_weight.astype(jnp.float32), output_weight.astype(jnp.float32), gateup_weight.astype(jnp.float32), down_weight.astype(jnp.float32), first_gain.astype(jnp.float32), second_gain.astype(jnp.float32), query_gain.astype(jnp.float32), key_gain.astype(jnp.float32))

    def forward(*weights):
        return layer(*weights, segments, positions)
    result, pull = jax.vjp(forward, *floats)
    grads = pull(cotangent.astype(jnp.float32))
    return (result.astype(jnp.bfloat16), grads[0].astype(jnp.bfloat16), grads[1], grads[2], grads[3], grads[4], grads[5], grads[6], grads[7], grads[8])
```

```python
import functools
import math

import jax
import jax.numpy as jnp
from jax import lax
from jax.experimental import pallas as pl
from jax.experimental.pallas import tpu as pltpu
from jax.sharding import PartitionSpec as P

MESH = pl.DeviceIdType.MESH


def places():
    dp, row, col = (lax.axis_index(n) for n in ("dp", "row", "col"))
    core = lax.rem(row, 2)
    far = 2 - 2 * (row // 2) + core
    sibling = row + 1 - 2 * core
    return row, far, sibling, (dp, far, col), (dp, row, 1 - col), (dp, sibling, col)


def greet(partners):
    barrier = pltpu.get_barrier_semaphore()
    for partner in partners:
        pl.semaphore_signal(barrier, inc=1, device_id=partner, device_id_type=MESH)
    pl.semaphore_wait(barrier, len(partners))


def gather_kernel(x_ref, o_ref, local_sem, send_sem, recv_sem):
    rows, width = x_ref.shape
    half = rows // 2
    row, far, sibling, xn, yn, sib = places()
    greet((xn, yn, sib))

    def at(block, part, other):
        start = block * rows if part is None else block * rows + part * half
        size = rows if part is None else half
        return o_ref.at[pl.ds(start, size), pl.ds(width if other else 0, width)]

    def send(index, src, dst, partner):
        copy = pltpu.make_async_remote_copy(
            src_ref=src, dst_ref=dst, send_sem=send_sem.at[index], recv_sem=recv_sem.at[index],
            device_id=partner, device_id_type=MESH)
        copy.start()
        return copy

    def mine(part):
        return x_ref.at[pl.ds(part * half, half)]

    x0 = send(0, mine(0), at(row, 0, False), xn)
    y1 = send(1, mine(1), at(row, 1, True), yn)
    x1 = send(2, mine(1), at(row, 1, False), xn)
    y0 = send(3, mine(0), at(row, 0, True), yn)
    s = send(4, x_ref, at(row, None, False), sib)
    own = pltpu.make_async_copy(x_ref, at(row, None, False), local_sem)
    own.start()
    x0.wait_recv()
    f0 = send(5, at(far, 0, False), at(far, 0, True), yn)
    s0 = send(7, at(far, 0, False), at(far, 0, False), sib)
    y1.wait_recv()
    f1 = send(6, at(row, 1, True), at(row, 1, True), xn)
    s1 = send(8, at(row, 1, True), at(row, 1, True), sib)
    x1.wait_recv()
    s2 = send(9, at(far, 1, False), at(far, 1, False), sib)
    y0.wait_recv()
    s3 = send(10, at(row, 0, True), at(row, 0, True), sib)
    f0.wait_recv()
    s4 = send(11, at(far, 0, True), at(far, 0, True), sib)
    f1.wait_recv()
    s5 = send(12, at(far, 1, True), at(far, 1, True), sib)
    own.wait()
    for copy in (s, s0, s1, s2, s3, s4, s5):
        copy.wait_recv()
    for copy in (x0, y1, x1, y0, s, f0, f1, s0, s1, s2, s3, s4, s5):
        copy.wait_send()


def gather_group(block, ident):
    rows, width = block.shape
    return pl.pallas_call(
        gather_kernel,
        out_shape=jax.ShapeDtypeStruct((4 * rows, 2 * width), block.dtype),
        in_specs=[pl.BlockSpec(memory_space=pltpu.VMEM)],
        out_specs=pl.BlockSpec(memory_space=pl.ANY),
        scratch_shapes=[pltpu.SemaphoreType.DMA, pltpu.SemaphoreType.DMA((13,)), pltpu.SemaphoreType.DMA((13,))],
        compiler_params=pltpu.CompilerParams(collective_id=ident, has_side_effects=True),
        cost_estimate=pl.CostEstimate(flops=0, bytes_accessed=50 * 1024 * 1024, transcendentals=0),
        name=f"gather{ident}",
    )(block)


def scatter_kernel(p_ref, o_ref, paired, out_buf, in_buf, send_sem, recv_sem):
    rows, width = o_ref.shape
    half = rows // 2
    row, far, sibling, xn, yn, sib = places()
    far_sibling = far + sibling - row
    greet((xn, yn, sib))

    def send(index, src, dst, partner):
        copy = pltpu.make_async_remote_copy(
            src_ref=src, dst_ref=dst, send_sem=send_sem.at[index], recv_sem=recv_sem.at[index],
            device_id=partner, device_id_type=MESH)
        copy.start()
        return copy

    def part(block, piece, other):
        return p_ref.at[pl.ds(block * rows + piece * half, half), pl.ds(width if other else 0, width)]

    plan = ((1, 0, 1), (1, 1, 1), (1, 0, 0), (1, 1, 0), (0, 0, 1), (0, 1, 1), (0, 0, 0), (0, 1, 0))
    order = (0, 1, 2, 5, 3, 4, 6, 7)
    swaps = {}
    for slot in order:
        away, piece, other = plan[slot]
        block = far_sibling if away else sibling
        swaps[slot] = send(slot, part(block, piece, other), paired.at[slot], sib)

    def total(slot):
        away, piece, other = plan[slot]
        swaps[slot].wait_recv()
        block = far if away else row
        mine = p_ref[pl.ds(block * rows + piece * half, half), pl.ds(width if other else 0, width)]
        return mine.astype(jnp.float32) + paired[slot].astype(jnp.float32)

    def push(slot, value, index, partner):
        out_buf[slot] = value.astype(out_buf.dtype)
        return send(index, out_buf.at[slot], in_buf.at[slot], partner)

    d0 = push(0, total(0), 8, xn)
    d1 = push(1, total(1), 9, yn)
    x0 = push(2, total(2), 10, xn)
    y1 = push(5, total(5), 13, yn)
    x_late, y_late = total(3), total(4)
    d1.wait_recv()
    x1 = push(3, x_late + in_buf[1].astype(jnp.float32), 11, xn)
    d0.wait_recv()
    y0 = push(4, y_late + in_buf[0].astype(jnp.float32), 12, yn)
    for piece, first, second in ((0, x0, y0), (1, x1, y1)):
        value = total(6 + piece)
        first.wait_recv()
        second.wait_recv()
        o_ref[pl.ds(piece * half, half), :] = (
            value + in_buf[2 + piece].astype(jnp.float32) + in_buf[4 + piece].astype(jnp.float32))
    for copy in (*swaps.values(), d0, d1, x0, y1, x1, y0):
        copy.wait_send()


def scatter_group(partial, ident):
    rows, width = partial.shape[0] // 4, partial.shape[1] // 2
    half = rows // 2
    return pl.pallas_call(
        scatter_kernel,
        out_shape=jax.ShapeDtypeStruct((rows, width), jnp.float32),
        in_specs=[pl.BlockSpec(memory_space=pltpu.VMEM)],
        out_specs=pl.BlockSpec(memory_space=pltpu.VMEM),
        scratch_shapes=[
            pltpu.VMEM((8, half, width), partial.dtype),
            pltpu.VMEM((6, half, width), partial.dtype),
            pltpu.VMEM((6, half, width), partial.dtype),
            pltpu.SemaphoreType.DMA((14,)), pltpu.SemaphoreType.DMA((14,))],
        compiler_params=pltpu.CompilerParams(collective_id=ident, has_side_effects=True),
        cost_estimate=pl.CostEstimate(flops=0, bytes_accessed=50 * 1024 * 1024, transcendentals=0),
        name=f"scatter{ident}",
    )(partial)


SEQ_LEN = 1024


epsilon = 1e-06
log_theta = math.log(1000000.0)


def col_total(values):
    return lax.psum(values, "col")


def gather_rows(values):
    return lax.all_gather(values, "row", axis=0, tiled=True)


def sum_rows(values):
    return lax.psum_scatter(values, "row", scatter_dimension=0, tiled=True)


def rms_norm(values, gain):
    return values * lax.rsqrt(jnp.mean(values * values, axis=-1, keepdims=True) + epsilon) * gain


def tables(positions, head_size):
    half_size = head_size // 2
    freqs = jnp.exp(-log_theta * jnp.arange(half_size).astype(jnp.float32) * 2.0 / head_size)
    angles = positions.astype(jnp.float32)[:, None] * freqs[None, :]
    return (jnp.cos(angles), jnp.sin(angles))


def rotate(values, cosine, sine):
    half_size = values.shape[-1] // 2
    first_half = values[..., :half_size]
    second_half = values[..., half_size:]
    return jnp.concatenate(
        [first_half * cosine - second_half * sine, second_half * cosine + first_half * sine],
        axis=-1,
    )


def norm_forward(values, gain, width):
    squares = col_total(jnp.sum(values * values, axis=1))
    factor = lax.rsqrt(squares / width + epsilon)
    return (values * factor[:, None] * gain, factor)


def norm_backward(values, gain, factor, upstream, width):
    scaled = upstream * gain
    inner_sum = col_total(jnp.sum(scaled * values, axis=1))
    result = (
        scaled * factor[:, None] - values * (factor * factor * factor * inner_sum / width)[:, None]
    )
    return (result, jnp.sum(upstream * values * factor[:, None], axis=0))


def swiglu(gate_up):
    half_size = gate_up.shape[1] // 2
    return jax.nn.silu(gate_up[:, :half_size]) * gate_up[:, half_size:]


def inner_rows(left, right):
    return lax.dot_general(
        left, right, (((0,), (0,)), ((), ())), preferred_element_type=jnp.float32
    )


def times_transpose(left, right):
    return lax.dot_general(
        left, right, (((1,), (1,)), ((), ())), preferred_element_type=jnp.float32
    )


def block_scores(block_query, block_key, query_segs, key_segs, first_row, scale):
    scores = (
        jnp.einsum("igd,jd->gij", block_query, block_key, preferred_element_type=jnp.float32)
        * scale
    )
    query_spot = first_row + jnp.arange(block_query.shape[0], dtype=jnp.int32)
    key_spot = jnp.arange(block_key.shape[0], dtype=jnp.int32)
    allowed = (key_spot[None, :] <= query_spot[:, None]) & (
        key_segs[None, :] == query_segs[:, None]
    )
    return jnp.where(allowed[None], scores, -1e30)


def block_slices(item, per_seq, block_rows, seq_len, queries, keys_all, values_all, segments):
    seq_start = item // per_seq * seq_len
    offset = item % per_seq * block_rows
    block_query = lax.dynamic_slice_in_dim(queries, seq_start + offset, block_rows, 0)
    query_segs = lax.dynamic_slice_in_dim(segments, seq_start + offset, block_rows, 0)
    return (block_query, keys_all, values_all, query_segs, segments, seq_start + offset, offset)


def attention_forward(queries, keys_all, values_all, segments, seq_len):
    row_count = queries.shape[0]
    block_rows = min(512, seq_len)
    per_seq = seq_len // block_rows
    scale = 1.0 / math.sqrt(queries.shape[-1])

    def one_block(item):
        block_query, block_key, block_value, query_segs, key_segs, start_row, offset = block_slices(
            item, per_seq, block_rows, seq_len, queries, keys_all, values_all, segments
        )
        scores = block_scores(block_query, block_key, query_segs, key_segs, offset, scale)
        peak = jnp.max(scores, axis=-1, keepdims=True)
        weights = jnp.exp(scores - peak)
        totals = jnp.sum(weights, axis=-1, keepdims=True)
        probs = (weights / totals).astype(jnp.bfloat16)
        mixed = jnp.einsum("gij,jd->igd", probs, block_value, preferred_element_type=jnp.float32)
        return (mixed, peak, totals)

    items = jnp.arange(row_count // seq_len * per_seq, dtype=jnp.int32)
    mixed, peak, totals = lax.map(one_block, items)
    return (mixed.reshape(row_count, mixed.shape[2] * mixed.shape[3]), peak, totals)


def attention_backward(queries, keys_all, values_all, segments, seq_len, peak, totals, upstream):
    row_count = queries.shape[0]
    head_size = queries.shape[-1]
    block_rows = min(512, seq_len)
    per_seq = seq_len // block_rows
    scale = 1.0 / math.sqrt(head_size)

    def one_block(packed_item):
        item, block_peak, block_total = packed_item
        block_query, block_key, block_value, query_segs, key_segs, start_row, offset = block_slices(
            item, per_seq, block_rows, seq_len, queries, keys_all, values_all, segments
        )
        scores = block_scores(block_query, block_key, query_segs, key_segs, offset, scale)
        probs = jnp.exp(scores - block_peak) / block_total
        probs_low = probs.astype(jnp.bfloat16)
        block_grad = lax.dynamic_slice_in_dim(upstream, start_row, block_rows, 0)
        dprobs = jnp.einsum(
            "igd,jd->gij", block_grad, block_value, preferred_element_type=jnp.float32
        )
        dscores = probs * (dprobs - jnp.sum(probs * dprobs, axis=-1, keepdims=True))
        dscores_low = dscores.astype(jnp.bfloat16)
        grad_query = (
            jnp.einsum("gij,jd->igd", dscores_low, block_key, preferred_element_type=jnp.float32)
            * scale
        )
        grad_key = (
            jnp.einsum("gij,igd->jd", dscores_low, block_query, preferred_element_type=jnp.float32)
            * scale
        )
        grad_value = jnp.einsum(
            "gij,igd->jd", probs_low, block_grad, preferred_element_type=jnp.float32
        )
        return (grad_query, grad_key, grad_value)

    items = jnp.arange(row_count // seq_len * per_seq, dtype=jnp.int32)
    grad_query, grad_key, grad_value = lax.map(one_block, (items, peak, totals))
    seq_count = row_count // seq_len
    grad_query = grad_query.reshape(row_count, 2, head_size)
    grad_key = jnp.sum(grad_key.reshape(seq_count, per_seq, seq_len, head_size), axis=1).reshape(
        row_count, head_size
    )
    grad_value = jnp.sum(
        grad_value.reshape(seq_count, per_seq, seq_len, head_size), axis=1
    ).reshape(row_count, head_size)
    return (grad_query, grad_key, grad_value)


def swap_col(values):
    return lax.ppermute(values, "col", [(0, 1), (1, 0)])


def token_norm(values, gain):
    wide = values.astype(jnp.float32)
    factor = lax.rsqrt(jnp.mean(wide * wide, axis=1, keepdims=True) + epsilon)
    return (wide * factor * gain).astype(jnp.bfloat16)


def per_device(
    inputs,
    heads_weight,
    output_weight,
    gateup_weight,
    down_weight,
    first_gain,
    second_gain,
    query_gain,
    key_gain,
    segments,
    positions,
    cotangent,
):
    head_size = query_gain.shape[0]
    col = lax.axis_index("col")
    half_width = inputs.shape[1]
    width = half_width * 2
    group_rows = segments.shape[0]
    seq_len = SEQ_LEN

    def halves(weight, axis):
        size = weight.shape[axis] // 2
        mine = lax.dynamic_slice_in_dim(weight, col * size, size, axis)
        theirs = lax.dynamic_slice_in_dim(weight, (1 - col) * size, size, axis)
        return mine, theirs

    def ordered(mine, theirs, axis):
        flag = col == 0
        return jnp.concatenate(
            [jnp.where(flag, mine, theirs), jnp.where(flag, theirs, mine)], axis=axis
        )

    heads_mine, heads_theirs = halves(heads_weight, 1)
    output_mine, output_theirs = halves(output_weight, 0)
    gateup_mine, gateup_theirs = halves(gateup_weight, 1)
    down_mine, down_theirs = halves(down_weight, 0)
    heads_got = swap_col(heads_theirs)
    output_got = swap_col(output_theirs)
    gateup_theirs, heads_got = lax.optimization_barrier((gateup_theirs, heads_got))
    gateup_got = swap_col(gateup_theirs)
    down_theirs, gateup_got = lax.optimization_barrier((down_theirs, gateup_got))
    down_got = swap_col(down_theirs)
    gain_rows = jnp.stack([first_gain, second_gain])
    gains_all = jnp.concatenate([gain_rows, swap_col(gain_rows)], axis=1)

    inputs_all = gather_group(inputs, 0)
    inputs_float = inputs.astype(jnp.float32)
    normed_all = token_norm(inputs_all, gains_all[0])
    heads_full = jnp.concatenate([heads_mine, heads_got], axis=0)
    packed = jnp.dot(normed_all, heads_full, preferred_element_type=jnp.float32)
    cosine, sine = tables(positions, head_size)

    def prepare(packed_part, gain_query, gain_key):
        pieces = packed_part.reshape(group_rows, 4, head_size)
        rotated_query = rotate(rms_norm(pieces[:, 0:2], gain_query), cosine[:, None], sine[:, None])
        rotated_key = rotate(rms_norm(pieces[:, 2], gain_key), cosine, sine)
        return (rotated_query, rotated_key, pieces[:, 3])

    (rotated_query, rotated_key, value_part), prepare_back = jax.vjp(
        prepare, packed, query_gain, key_gain
    )
    query_low = rotated_query.astype(jnp.bfloat16)
    key_low = rotated_key.astype(jnp.bfloat16)
    value_low = value_part.astype(jnp.bfloat16)
    attended, peak, totals = attention_forward(query_low, key_low, value_low, segments, seq_len)
    attended = attended.astype(jnp.bfloat16)
    output_full = jnp.concatenate([output_mine, output_got], axis=1)
    branch = jnp.dot(attended, output_full, preferred_element_type=jnp.float32)
    middle = inputs_float + scatter_group(branch.astype(jnp.bfloat16), 1)
    normed_two, second_factor = norm_forward(middle, second_gain, width)
    normed_two_all = gather_group(normed_two.astype(jnp.bfloat16), 2)
    gateup_full = jnp.concatenate([gateup_mine, gateup_got], axis=0)
    gate_up = jnp.dot(normed_two_all, gateup_full, preferred_element_type=jnp.float32)
    hidden, swiglu_back = jax.vjp(swiglu, gate_up)
    hidden = hidden.astype(jnp.bfloat16)
    hidden_got = swap_col(hidden)
    attended_got = swap_col(attended)
    upstream_all = gather_group(cotangent, 3)
    down_full = jnp.concatenate([down_mine, down_got], axis=1)
    grad_hidden = times_transpose(upstream_all, down_full)
    grad_gate_up = swiglu_back(grad_hidden)[0].astype(jnp.bfloat16)
    grad_gate_up_got = swap_col(grad_gate_up)
    down_part = inner_rows(ordered(hidden, hidden_got, 1), upstream_all[:, :half_width])
    grad_normed_two = scatter_group(
        times_transpose(grad_gate_up, gateup_full).astype(jnp.bfloat16), 4
    )
    grad_back_two, second_part = norm_backward(
        middle, second_gain, second_factor, grad_normed_two, width
    )
    grad_middle = cotangent.astype(jnp.float32) + grad_back_two
    middle_all = gather_group(grad_middle.astype(jnp.bfloat16), 5)
    grad_attended = times_transpose(middle_all, output_full)
    gateup_part = inner_rows(
        normed_two_all[:, :half_width], ordered(grad_gate_up, grad_gate_up_got, 1)
    )
    grad_attended_low = grad_attended.astype(jnp.bfloat16).reshape(group_rows, 2, head_size)
    grad_query, grad_key, grad_value = attention_backward(
        query_low, key_low, value_low, segments, seq_len, peak, totals, grad_attended_low
    )
    grad_packed, query_part, key_part = prepare_back((grad_query, grad_key, grad_value))
    grad_packed = grad_packed.astype(jnp.bfloat16)
    grad_packed_got = swap_col(grad_packed)
    output_part = inner_rows(ordered(attended, attended_got, 1), middle_all[:, :half_width])
    grad_normed = scatter_group(times_transpose(grad_packed, heads_full).astype(jnp.bfloat16), 6)
    squares = col_total(jnp.sum(inputs_float * inputs_float, axis=1))
    first_factor = lax.rsqrt(squares / width + epsilon)
    grad_back_one, first_part = norm_backward(
        inputs_float, first_gain, first_factor, grad_normed, width
    )
    input_grad = (grad_middle + grad_back_one).astype(jnp.bfloat16)
    heads_part = inner_rows(
        normed_all[:, :half_width], ordered(grad_packed, grad_packed_got, 1)
    )
    result = middle + scatter_group(
        jnp.dot(hidden, down_full, preferred_element_type=jnp.float32).astype(jnp.bfloat16), 7
    )

    def total(part):
        return lax.psum(part.astype(jnp.bfloat16), "dp").astype(jnp.float32)

    down_grad = total(down_part)
    gateup_grad = total(gateup_part)
    output_grad = total(output_part)
    heads_grad = total(heads_part)
    place = col * first_gain.shape[0]
    blank = jnp.zeros((width,), jnp.float32)
    first_full = lax.dynamic_update_slice_in_dim(blank, first_part, place, 0)
    second_full = lax.dynamic_update_slice_in_dim(blank, second_part, place, 0)
    first_sum, second_sum, querygain_grad, keygain_grad = lax.psum(
        (first_full, second_full, query_part, key_part), ("dp", "row", "col")
    )
    first_grad = lax.dynamic_slice_in_dim(first_sum, place, first_gain.shape[0], 0)
    second_grad = lax.dynamic_slice_in_dim(second_sum, place, second_gain.shape[0], 0)
    return (
        result.astype(jnp.bfloat16),
        input_grad,
        heads_grad,
        output_grad,
        gateup_grad,
        down_grad,
        first_grad,
        second_grad,
        querygain_grad,
        keygain_grad,
    )


def solution(mesh):
    placed = (
        P(("dp", "row"), "col"),
        P("col", "row"),
        P("row", "col"),
        P("col", "row"),
        P("row", "col"),
        P("col"),
        P("col"),
        P(),
        P(),
        P("dp"),
        P("dp"),
        P(("dp", "row"), "col"),
    )
    return jax.shard_map(
        per_device,
        mesh=mesh,
        in_specs=placed,
        out_specs=(
            P(("dp", "row"), "col"),
            P(("dp", "row"), "col"),
            P("col", "row"),
            P("row", "col"),
            P("col", "row"),
            P("row", "col"),
            P("col"),
            P("col"),
            P(),
            P(),
        ),
        check_vma=False,
    )
```
